128 devices in a mesh: nodes: 128 (over z, y, x, core).
Axes of the slice: x: 4, y: 4, z: 4, core: 2. Of those that a mesh axis runs over, the one named last changes fastest.
Arguments:
- adjacency: bfloat16 [16384, 16384], P('nodes')
- features: bfloat16 [16384, 1433], P('nodes')
- w_hidden: float32 [1433, 16], replicated
- w_output: float32 [16, 7], replicated
- labels: int32 [16384], P('nodes')
- train_mask: int32 [16384], P('nodes')
- block_mask: int32 [128, 128], replicated
Outputs:
- output 1: float32 [], replicated
- output 2: float32 [1433, 16], replicated
- output 3: float32 [16, 7], replicated
All inputs are finite; a program needn't handle non-finite values.
Results may differ from the reference program's by a relative error of at most 0.001.
Values are sent between devices in bfloat16 or wider.
A program may use at most 1 GiB of HBM per device.

```python
import jax
import jax.numpy as jnp
from jax import lax

NUM_NODES = 16384
BLOCKS = 128
F_IN = 1433
HID = 16
CLASSES = 7
EDGE_PERCENT = 15
BLOCK_ROWS = NUM_NODES // BLOCKS


def setup_inputs(seed: int = 0) -> dict:
    keys = jax.random.split(jax.random.key(seed), 9)
    thresholds = jax.random.randint(keys[0], (BLOCKS, 1), BLOCKS // 8, BLOCKS + 1, dtype=jnp.int32)
    block_draw = jax.random.randint(keys[1], (BLOCKS, BLOCKS), 0, BLOCKS, dtype=jnp.int32)
    block_mask = jnp.maximum((block_draw < thresholds).astype(jnp.int32), jnp.eye(BLOCKS, dtype=jnp.int32))
    col_ids = jnp.arange(NUM_NODES, dtype=jnp.int32)

    def edge_rows(block_id):
        edge_draw = jax.random.randint(jax.random.fold_in(keys[2], block_id), (BLOCK_ROWS, NUM_NODES), 0, 100, dtype=jnp.int32)
        row_ids = block_id * BLOCK_ROWS + jnp.arange(BLOCK_ROWS, dtype=jnp.int32)
        col_keep = jnp.repeat(block_mask[block_id], BLOCK_ROWS) > 0
        edge_on = ((edge_draw < EDGE_PERCENT) | (row_ids[:, None] == col_ids[None, :])) & col_keep[None, :]
        raw_weight = edge_on.astype(jnp.float32)
        return (raw_weight / jnp.sum(raw_weight, axis=1, keepdims=True)).astype(jnp.bfloat16)

    adjacency = lax.map(edge_rows, jnp.arange(BLOCKS, dtype=jnp.int32)).reshape(NUM_NODES, NUM_NODES)
    centers = jax.random.normal(keys[3], (BLOCKS, F_IN), jnp.float32)
    noise = jax.random.normal(keys[4], (NUM_NODES, F_IN), jnp.float32)
    features = (jnp.repeat(centers, BLOCK_ROWS, axis=0) + noise).astype(jnp.bfloat16)
    w_hidden = jax.random.normal(keys[5], (F_IN, HID), jnp.float32) * (F_IN ** -0.5 * BLOCKS ** 0.25)
    w_output = jax.random.normal(keys[6], (HID, CLASSES), jnp.float32) * (2.0 * HID ** -0.5)
    labels = jax.random.randint(keys[7], (NUM_NODES,), 0, CLASSES, dtype=jnp.int32)
    label_draw = jax.random.randint(keys[8], (NUM_NODES,), 0, 100, dtype=jnp.int32)
    train_mask = jnp.maximum((label_draw < 40).astype(jnp.int32), (col_ids == 0).astype(jnp.int32))
    return dict(adjacency=adjacency, features=features, w_hidden=w_hidden, w_output=w_output, labels=labels, train_mask=train_mask, block_mask=block_mask)


def masked_product(adj_blocks, block_mask, values):
    width = values.shape[-1]
    value_blocks = values.reshape(BLOCKS, BLOCK_ROWS, width)

    def one_block(block_item):
        adj_rows, mask_row = block_item
        scaled = value_blocks * mask_row.astype(values.dtype)[:, None, None]
        return jnp.dot(adj_rows, scaled.reshape(NUM_NODES, width), preferred_element_type=jnp.float32)

    return lax.map(one_block, (adj_blocks, block_mask)).reshape(NUM_NODES, width)


def masked_transpose_product(adj_blocks, block_mask, grads):
    width = grads.shape[-1]
    grad_blocks = grads.reshape(BLOCKS, BLOCK_ROWS, width)

    def add_block(running_sum, block_item):
        adj_rows, mask_row, grad_rows = block_item
        contrib = jnp.dot(adj_rows.T, grad_rows, preferred_element_type=jnp.float32)
        contrib = contrib.reshape(BLOCKS, BLOCK_ROWS, width) * mask_row.astype(jnp.float32)[:, None, None]
        return running_sum + contrib.reshape(NUM_NODES, width), None

    start_sum = jnp.zeros((NUM_NODES, width), jnp.float32)
    total_sum, _ = lax.scan(add_block, start_sum, (adj_blocks, block_mask, grad_blocks))
    return total_sum


def reference(adjacency, features, w_hidden, w_output, labels, train_mask, block_mask):
    adj_blocks = adjacency.reshape(BLOCKS, BLOCK_ROWS, NUM_NODES)
    w_hidden_bf = w_hidden.astype(jnp.bfloat16)
    w_output_bf = w_output.astype(jnp.bfloat16)
    proj_one = jnp.dot(features, w_hidden_bf, preferred_element_type=jnp.float32).astype(jnp.bfloat16)
    agg_one = masked_product(adj_blocks, block_mask, proj_one)
    hidden = jnp.maximum(agg_one, 0.0).astype(jnp.bfloat16)
    proj_two = jnp.dot(hidden, w_output_bf, preferred_element_type=jnp.float32).astype(jnp.bfloat16)
    logits = masked_product(adj_blocks, block_mask, proj_two)
    label_weight = train_mask.astype(jnp.float32)
    label_count = jnp.sum(label_weight)
    log_norm = jax.nn.logsumexp(logits, axis=-1)
    one_hot = (labels[:, None] == jnp.arange(CLASSES)[None, :]).astype(jnp.float32)
    picked = jnp.sum(logits * one_hot, axis=-1)
    mean_loss = jnp.sum(label_weight * (log_norm - picked)) / label_count
    probabilities = jnp.exp(logits - log_norm[:, None])
    grad_logits = ((probabilities - one_hot) * (label_weight / label_count)[:, None]).astype(jnp.bfloat16)
    grad_proj_two = masked_transpose_product(adj_blocks, block_mask, grad_logits).astype(jnp.bfloat16)
    grad_w_output = jnp.dot(hidden.T, grad_proj_two, preferred_element_type=jnp.float32)
    grad_hidden = jnp.dot(grad_proj_two, w_output_bf.T, preferred_element_type=jnp.float32)
    grad_agg = jnp.where(agg_one > 0, grad_hidden, 0.0).astype(jnp.bfloat16)
    grad_proj_one = masked_transpose_product(adj_blocks, block_mask, grad_agg).astype(jnp.bfloat16)
    grad_w_hidden = jnp.dot(features.T, grad_proj_one, preferred_element_type=jnp.float32)
    return (mean_loss, grad_w_hidden, grad_w_output)
```

```python
import functools

import jax
import jax.numpy as jnp
from jax import lax
from jax.experimental import pallas as pl
from jax.experimental.pallas import tpu as pltpu
from jax.sharding import PartitionSpec as P

AXIS = 'nodes'
MESH = pl.DeviceIdType.MESH
BF = jnp.bfloat16
F32 = jnp.float32
NT = (((1,), (1,)), ((), ()))
TN = (((0,), (0,)), ((), ()))
B = 128
CLS = 7


def kernel(R, adj, x_t, wh_t, wo_t, labels, tmask, bmask, gwh_out, gwo_out, loss_out,
           a_v, x_v, wh_v, wo_v, wo_pad, lab_v, tm_v, bm_s, y1_v, y2_v, z_v, z_rx,
           g_v, e_v, p_v, p_rx, q_v, q_rx, part, part_rx, acc, acc_rx, fin_rx,
           load_sem, a_sem, a_send, d_send, d_recv, send_sem, recv_sem, ar_send, ar_recv):
    NC = R * R * R
    f_in = x_v.shape[0]
    fpad = part.shape[2] - B
    me = lax.axis_index(AXIS)
    core = lax.rem(me, 2)
    chip = lax.div(me, 2)
    cx = lax.rem(chip, R)
    cy = lax.rem(lax.div(chip, R), R)
    cz = lax.div(chip, R * R)
    partner = chip * 2 + (1 - core)

    def peer(dz, dy, dx):
        tz = lax.rem(cz + dz, R)
        ty = lax.rem(cy + dy, R)
        tx = lax.rem(cx + dx, R)
        return (tz * R + ty) * R + tx

    def peer_k(k):
        return peer(lax.div(k, R * R), lax.rem(lax.div(k, R), R), lax.rem(k, R))

    def blk(t):
        return pl.ds(pl.multiple_of(t * B, B), B)

    small = [
        pltpu.make_async_copy(x_t, x_v, load_sem.at[0]),
        pltpu.make_async_copy(wh_t, wh_v, load_sem.at[1]),
        pltpu.make_async_copy(wo_t, wo_v, load_sem.at[2]),
        pltpu.make_async_copy(labels, lab_v, load_sem.at[3]),
        pltpu.make_async_copy(tmask, tm_v, load_sem.at[4]),
        pltpu.make_async_copy(bmask.at[pl.ds(pl.multiple_of(lax.div(2 * chip, 8) * 8, 8), 8), :], bm_s, load_sem.at[5]),
    ]
    for c in small:
        c.start()

    barrier = pltpu.get_barrier_semaphore()

    def greet(k, _):
        pl.semaphore_signal(barrier, inc=1, device_id=(peer_k(k) * 2 + core,), device_id_type=MESH)
        return 0

    lax.fori_loop(1, NC, greet, 0)
    pl.semaphore_signal(barrier, inc=1, device_id=(partner,), device_id_type=MESH)

    my_rows = pl.ds(pl.multiple_of(core * B, B), B)

    def load_a(t, _):
        pltpu.make_async_copy(adj.at[:, blk(2 * t + core)], a_v.at[my_rows, blk(t)], a_sem.at[0]).start()
        return 0

    lax.fori_loop(0, NC, load_a, 0)

    wo_pad[...] = jnp.zeros_like(wo_pad)
    g_v[...] = jnp.zeros_like(g_v)
    part[...] = jnp.zeros_like(part)
    small[0].wait()
    small[1].wait()
    y1 = jnp.dot(wh_v[...].astype(BF), x_v[...], preferred_element_type=F32).astype(BF)
    y1_v[:, blk(chip)] = y1

    pl.semaphore_wait(barrier, NC)

    def gather_start(buf, i):
        def send(k, _):
            pltpu.make_async_remote_copy(
                src_ref=buf.at[:, blk(chip)], dst_ref=buf.at[:, blk(chip)], send_sem=send_sem.at[i], recv_sem=recv_sem.at[i],
                device_id=(peer_k(k) * 2 + core,), device_id_type=MESH).start()
            return 0

        lax.fori_loop(1, NC, send, 0)

    def wait_all(ref, sem):
        pltpu.make_async_copy(ref, ref, sem).wait()

    gather_start(y1_v, 0)

    def swap_a(t, _):
        pltpu.make_async_remote_copy(
            src_ref=adj.at[:, blk(2 * t + 1 - core)], dst_ref=a_v.at[my_rows, blk(t)], send_sem=a_send, recv_sem=a_sem.at[1],
            device_id=(partner,), device_id_type=MESH).start()
        return 0

    lax.fori_loop(0, NC, swap_a, 0)
    for c in small[2:]:
        c.wait()
    wo_pad[0:CLS, :] = wo_v[...]
    wo_bf = wo_pad[...].astype(BF)
    wait_all(a_v.at[0:B, :], a_sem.at[0])
    wait_all(a_v.at[0:B, :], a_sem.at[1])

    row0 = lax.rem(2 * chip, 8)

    def mask_block(t, _):
        for h in range(2):
            m = bm_s[row0 + h, 2 * t + core].astype(F32)
            m_vec = jnp.full((B, B), m, F32).astype(BF)
            a_v[h * B:(h + 1) * B, blk(t)] = a_v[h * B:(h + 1) * B, blk(t)] * m_vec
        return 0

    lax.fori_loop(0, NC, mask_block, 0)

    def to_partner(src, dst, i):
        return pltpu.make_async_remote_copy(src_ref=src, dst_ref=dst, send_sem=d_send.at[i], recv_sem=d_recv.at[i],
                                            device_id=(partner,), device_id_type=MESH)

    def others(buf):
        return buf.at[:, 0:(NC - 1) * B]

    wait_all(others(y1_v), recv_sem.at[0])
    zp = lax.dot_general(y1_v[...], a_v[...], NT, preferred_element_type=F32)
    z_v[0, 0] = zp[:, 0:B]
    z_v[0, 1] = zp[:, B:2 * B]
    zc = to_partner(z_v.at[0, 1 - core], z_rx.at[0], 0)
    zc.start()
    zc.wait()
    z1 = z_v[0, core] + z_rx[0]
    h_bf = jnp.maximum(z1, 0.0).astype(BF)
    rows16 = lax.broadcasted_iota(jnp.int32, (16, B), 0)
    m_row = tm_v[...].astype(F32)
    y2 = jnp.dot(wo_bf, h_bf, preferred_element_type=F32)
    y2 = jnp.where(rows16 == CLS, m_row, y2)
    y2_v[:, blk(chip)] = y2.astype(BF)
    gather_start(y2_v, 1)

    wait_all(others(y2_v), recv_sem.at[1])
    zp = lax.dot_general(y2_v[...], a_v[...], NT, preferred_element_type=F32)
    cnt = jnp.zeros((16, B), F32)
    for t in range(NC):
        cnt = cnt + y2_v[:, t * B:(t + 1) * B].astype(F32)
    z_v[1, 0] = jnp.where(rows16 == CLS, cnt, zp[:, 0:B])
    z_v[1, 1] = jnp.where(rows16 == CLS, cnt, zp[:, B:2 * B])
    zc2 = to_partner(z_v.at[1, 1 - core], z_rx.at[1], 1)
    zc2.start()
    zc2.wait()
    z2 = (z_v[1, core] + z_rx[1])[0:8, :]
    rows8 = lax.broadcasted_iota(jnp.int32, (8, B), 0)
    count = jnp.sum(z2[CLS:CLS + 1, :], axis=1, keepdims=True)
    valid = rows8 < CLS
    zmax = jnp.max(jnp.where(valid, z2, -jnp.inf), axis=0, keepdims=True)
    esum = jnp.sum(jnp.where(valid, jnp.exp(z2 - zmax), 0.0), axis=0, keepdims=True)
    log_norm = jnp.log(esum) + zmax
    hot = rows8 == lab_v[...]
    picked = jnp.sum(jnp.where(hot, z2, 0.0), axis=0, keepdims=True)
    loss_part = jnp.sum(m_row * (log_norm - picked), axis=1, keepdims=True)
    prob = jnp.exp(jnp.where(valid, z2 - log_norm, 0.0))
    g = (prob - hot.astype(F32)) * (m_row / count)
    g = jnp.where(valid, g, 0.0)
    g_v[:, blk(core)] = jnp.concatenate([g, jnp.zeros_like(g)], axis=0).astype(BF)
    gc = to_partner(g_v.at[:, blk(core)], g_v.at[:, blk(core)], 2)
    gc.start()
    gc.wait()

    def scatter_product(lhs_v, rows, out_v, rx, i):
        lhs = lhs_v[...]
        W = R * B

        def one_group(dz, dy, first_x):
            base = (lax.rem(cz + dz, R) * R + lax.rem(cy + dy, R)) * R
            res = jnp.dot(lhs, a_v[:, pl.ds(pl.multiple_of(base * B, W), W)], preferred_element_type=F32)
            for j in range(R):
                out_v[base + j] = res[0:rows, j * B:(j + 1) * B]
            for dx in range(first_x, R):
                t = base + lax.rem(cx + dx, R)
                pltpu.make_async_remote_copy(
                    src_ref=out_v.at[t], dst_ref=rx.at[chip], send_sem=send_sem.at[i], recv_sem=recv_sem.at[i],
                    device_id=(t * 2 + core,), device_id_type=MESH).start()

        def step(k, _):
            one_group(lax.div(k, R), lax.rem(k, R), 0)
            return 0

        lax.fori_loop(1, R * R, step, 0)
        one_group(0, 0, 1)
        rx[chip] = out_v[chip]
        wait_all(rx.at[0:NC - 1], recv_sem.at[i])
        return jnp.sum(rx[...], axis=0)

    d2 = scatter_product(g_v, 8, p_v, p_rx, 2).astype(BF)
    d2_16 = jnp.concatenate([d2.astype(F32), jnp.zeros((8, B), F32)], axis=0).astype(BF)
    gh = lax.dot_general(wo_bf, d2_16, TN, preferred_element_type=F32)
    e_v[:, blk(core)] = jnp.where(z1 > 0, gh, 0.0).astype(BF)
    ec = to_partner(e_v.at[:, blk(core)], e_v.at[:, blk(core)], 3)
    ec.start()
    gwo = lax.dot_general(d2_16, h_bf, NT, preferred_element_type=F32)
    tail = jnp.where(rows8 == CLS, loss_part, 0.0)
    for h in range(2):
        part[h, :, fpad:] = tail
        part[h, :, fpad:fpad + 16] = jnp.where(rows8[:, 0:16] == CLS, loss_part, gwo[0:8, :])
    ec.wait()
    d1 = scatter_product(e_v, 16, q_v, q_rx, 3).astype(BF)
    gwh = lax.dot_general(d1, x_v[...], NT, preferred_element_type=F32)
    part[0, :, 0:f_in] = gwh[0:8]
    part[1, :, 0:f_in] = gwh[8:16]
    pc = to_partner(part.at[1 - core], part_rx, 4)
    pc.start()
    pc.wait()
    acc[0] = part[core] + part_rx[...]

    tiles = acc.shape[2] // B
    cuts = [0, tiles // 3 * B, 2 * (tiles // 3) * B, tiles * B]
    coords = (cz, cy, cx)

    def axis_peer(ax, d):
        off = [0, 0, 0]
        off[ax] = d
        return peer(*off) * 2 + core

    def cols(s):
        return slice(cuts[s], cuts[s + 1])

    def launch(p, s):
        ax = (p + s) % 3
        for d in range(1, R):
            pltpu.make_async_remote_copy(
                src_ref=acc.at[p, :, cols(s)], dst_ref=acc_rx.at[p, coords[ax], :, cols(s)],
                send_sem=ar_send.at[p, s], recv_sem=ar_recv.at[p, s],
                device_id=(axis_peer(ax, d),), device_id_type=MESH).start()
        acc_rx[p, coords[ax], :, cols(s)] = acc[p, :, cols(s)]

    for s in range(3):
        launch(0, s)
    for p in range(3):
        for s in range(3):
            wait_all(acc_rx.at[p, 0:R - 1, :, cols(s)], ar_recv.at[p, s])
            tot = acc_rx[p, 0, :, cols(s)]
            for r in range(1, R):
                tot = tot + acc_rx[p, r, :, cols(s)]
            acc[p + 1, :, cols(s)] = tot
            if p < 2:
                launch(p + 1, s)
    fc = to_partner(acc.at[3], fin_rx, 5)
    fc.start()
    gwo_out[...] = acc[3, 0:CLS, fpad:fpad + 16]
    loss_out[...] = acc[3, CLS:CLS + 1, fpad:fpad + 1] / count
    gwh_out[pl.ds(pl.multiple_of(core * 8, 8), 8), :] = acc[3, :, 0:f_in]
    fc.wait()
    gwh_out[pl.ds(pl.multiple_of((1 - core) * 8, 8), 8), :] = fin_rx[:, 0:f_in]

    wait_all(a_v.at[0:B, :], a_send)
    wait_all(others(y1_v), send_sem.at[0])
    wait_all(others(y2_v), send_sem.at[1])
    wait_all(p_rx.at[0:NC - 1], send_sem.at[2])
    wait_all(q_rx.at[0:NC - 1], send_sem.at[3])
    for p in range(3):
        for s in range(3):
            wait_all(acc_rx.at[p, 0:R - 1, :, cols(s)], ar_send.at[p, s])


def device_step(R, adj, feat, w_hidden, w_output, labels, train_mask, block_mask):
    NC = R * R * R
    f_in, hid = w_hidden.shape
    fpad = -(-f_in // B) * B
    any_spec = pl.BlockSpec(memory_space=pl.ANY)
    vmem_spec = pl.BlockSpec(memory_space=pltpu.VMEM)
    gwh, gwo, loss = pl.pallas_call(
        functools.partial(kernel, R),
        out_shape=(jax.ShapeDtypeStruct((hid, f_in), F32), jax.ShapeDtypeStruct((CLS, hid), F32), jax.ShapeDtypeStruct((1, 1), F32)),
        in_specs=[any_spec] * 7,
        out_specs=(vmem_spec, vmem_spec, vmem_spec),
        scratch_shapes=[
            pltpu.VMEM((2 * B, NC * B), BF),
            pltpu.VMEM((f_in, B), BF),
            pltpu.VMEM((hid, f_in), F32),
            pltpu.VMEM((CLS, hid), F32),
            pltpu.VMEM((16, hid), F32),
            pltpu.VMEM((1, B), jnp.int32),
            pltpu.VMEM((1, B), jnp.int32),
            pltpu.SMEM((8, block_mask.shape[1]), jnp.int32),
            pltpu.VMEM((hid, NC * B), BF),
            pltpu.VMEM((16, NC * B), BF),
            pltpu.VMEM((2, 2, 16, B), F32),
            pltpu.VMEM((2, 16, B), F32),
            pltpu.VMEM((16, 2 * B), BF),
            pltpu.VMEM((16, 2 * B), BF),
            pltpu.VMEM((NC, 8, B), F32),
            pltpu.VMEM((NC, 8, B), F32),
            pltpu.VMEM((NC, 16, B), F32),
            pltpu.VMEM((NC, 16, B), F32),
            pltpu.VMEM((2, 8, fpad + B), F32),
            pltpu.VMEM((8, fpad + B), F32),
            pltpu.VMEM((4, 8, fpad + B), F32),
            pltpu.VMEM((3, R, 8, fpad + B), F32),
            pltpu.VMEM((8, fpad + B), F32),
            pltpu.SemaphoreType.DMA((6,)),
            pltpu.SemaphoreType.DMA((2,)),
            pltpu.SemaphoreType.DMA,
            pltpu.SemaphoreType.DMA((6,)),
            pltpu.SemaphoreType.DMA((6,)),
            pltpu.SemaphoreType.DMA((4,)),
            pltpu.SemaphoreType.DMA((4,)),
            pltpu.SemaphoreType.DMA((3, 3)),
            pltpu.SemaphoreType.DMA((3, 3)),
        ],
        compiler_params=pltpu.CompilerParams(collective_id=0, has_side_effects=True, vmem_limit_bytes=60 * 1024 * 1024),
        name='gcn_step',
    )(adj, feat.T, w_hidden.T, w_output.T, labels.reshape(1, -1), train_mask.reshape(1, -1), block_mask)
    return loss[0, 0], gwh.T, gwo.T


def solution(mesh):
    row_spec = P(AXIS, None)
    vec_spec = P(AXIS)
    R = 4 if mesh.shape[AXIS] == 128 else 2
    return jax.shard_map(functools.partial(device_step, R), mesh=mesh,
                         in_specs=(row_spec, row_spec, P(), P(), vec_spec, vec_spec, P()), out_specs=(P(), P(), P()), check_vma=False)
```

```python
import functools

import jax
import jax.numpy as jnp
from jax import lax
from jax.experimental import pallas as pl
from jax.experimental.pallas import tpu as pltpu
from jax.sharding import PartitionSpec as P

AXIS = 'nodes'
MESH = pl.DeviceIdType.MESH
BF = jnp.bfloat16
F32 = jnp.float32
NT = (((1,), (1,)), ((), ()))
TN = (((0,), (0,)), ((), ()))
B = 128
CLS = 7


def kernel(R, adj, x_t, wh_t, wo_t, labels, tmask, bmask, gwh_out, gwo_out, loss_out,
           a_v, x_v, wh_v, wo_v, wo_pad, lab_v, tm_v, bm_s, y1_v, y2_v, z1_v, z1_rx, z2_v, z2_rx,
           g_v, e_v, p_v, p_rx, q_v, q_rx, part, rx0, acc1, rx1, acc2, rx2,
           load_sem, a_sem, a_send, d_send, d_recv, send_sem, recv_sem, ar_send, ar_recv):
    NC = R * R * R
    SL = R * R
    FAR = (2, 3, 1, 0) if R == 4 else (1, 0)
    NEAR = FAR[::-1]
    f_in = x_v.shape[0]
    width = part.shape[2]
    fpad = width - B
    me = lax.axis_index(AXIS)
    core = lax.rem(me, 2)
    other = 1 - core
    chip = lax.div(me, 2)
    cx = lax.rem(chip, R)
    cy = lax.rem(lax.div(chip, R), R)
    cz = lax.div(chip, SL)
    coords = (cz, cy, cx)
    partner = chip * 2 + other
    tz = [lax.rem(cz + d, R) * SL for d in range(R)]
    ty = [lax.rem(cy + d, R) * R for d in range(R)]
    tx = [lax.rem(cx + d, R) for d in range(R)]
    offsets = [(dz, dy, dx) for dz in FAR for dy in FAR for dx in FAR if dz or dy or dx]
    dz2 = [t * 2 + core for t in tz]
    dy2 = [t * 2 for t in ty]
    dx2 = [t * 2 for t in tx]

    def dev(dz, dy, dx):
        return dz2[dz] + dy2[dy] + dx2[dx]

    def blk(t):
        return pl.ds(pl.multiple_of(t * B, B), B)

    def rcopy(src, dst, ss, rs, device):
        return pltpu.make_async_remote_copy(src_ref=src, dst_ref=dst, send_sem=ss, recv_sem=rs, device_id=(device,), device_id_type=MESH)

    def wait_all(ref, sem):
        pltpu.make_async_copy(ref, ref, sem).wait()

    def ring_dev(ax, d, h):
        off = [0, 0, 0]
        off[ax] = d
        return (tz[off[0]] + ty[off[1]] + tx[off[2]]) * 2 + h

    barrier = pltpu.get_barrier_semaphore()
    for o in offsets:
        pl.semaphore_signal(barrier, inc=1, device_id=(dev(*o),), device_id_type=MESH)
    pl.semaphore_signal(barrier, inc=1, device_id=(partner,), device_id_type=MESH)
    for ax in range(3):
        for d in range(1, R):
            pl.semaphore_signal(barrier, inc=1, device_id=(ring_dev(ax, d, other),), device_id_type=MESH)

    mine = blk(core)
    theirs = blk(other)
    small = [
        pltpu.make_async_copy(x_t, x_v, load_sem.at[0]),
        pltpu.make_async_copy(wh_t, wh_v, load_sem.at[1]),
        pltpu.make_async_copy(bmask.at[pl.ds(pl.multiple_of(lax.div(2 * chip, 8) * 8, 8), 8), :], bm_s, load_sem.at[2]),
        pltpu.make_async_copy(wo_t, wo_v, load_sem.at[3]),
        pltpu.make_async_copy(labels, lab_v.at[:, mine], load_sem.at[4]),
        pltpu.make_async_copy(tmask, tm_v.at[:, mine], load_sem.at[5]),
    ]
    for c in small:
        c.start()

    def load_a(t, _):
        pltpu.make_async_copy(adj.at[:, blk(2 * t + core)], a_v.at[mine, blk(t)], a_sem.at[0]).start()
        return 0

    lax.fori_loop(0, NC, load_a, 0, unroll=4)
    wo_pad[...] = jnp.zeros_like(wo_pad)
    part[...] = jnp.zeros_like(part)
    small[0].wait()
    small[1].wait()
    y1_v[:, blk(chip)] = jnp.dot(wh_v[...].astype(BF), x_v[...], preferred_element_type=F32).astype(BF)
    for c in small[2:]:
        c.wait()
    wo_pad[0:CLS, :] = wo_v[...]
    wo_bf = wo_pad[...].astype(BF)

    row0 = lax.rem(2 * chip, 8)

    def mask_rows(h):
        def step(t, _):
            m = jnp.full((B, B), bm_s[row0 + h, 2 * t + core].astype(F32), F32).astype(BF)
            a_v[blk(h), blk(t)] = a_v[blk(h), blk(t)] * m
            return 0

        lax.fori_loop(0, NC, step, 0, unroll=4)

    wait_all(a_v.at[0:B, :], a_sem.at[0])
    mask_rows(core)

    pl.semaphore_wait(barrier, NC + 3 * (R - 1))

    def gather_start(buf, i):
        src = buf.at[:, blk(chip)]
        for o in offsets:
            rcopy(src, src, send_sem.at[i], recv_sem.at[i, o[0]], dev(*o)).start()

    gather_start(y1_v, 0)

    def swap_a(t, _):
        rcopy(adj.at[:, blk(2 * t + other)], a_v.at[mine, blk(t)], a_send, a_sem.at[1], partner).start()
        return 0

    lax.fori_loop(0, NC, swap_a, 0, unroll=4)
    lc = rcopy(labels, lab_v.at[:, mine], d_send.at[3], d_recv.at[3], partner)
    mc = rcopy(tmask, tm_v.at[:, mine], d_send.at[4], d_recv.at[4], partner)
    lc.start()
    mc.start()
    wait_all(a_v.at[0:B, :], a_sem.at[1])
    mask_rows(other)

    def slab(dz):
        z = lax.rem(cz + R - dz, R)
        return pl.ds(pl.multiple_of(z * (SL * B), SL * B), SL * B)

    def wait_slab(buf, i, dz):
        n = SL if dz else SL - 1
        wait_all(buf.at[:, 0:n * B], recv_sem.at[i, dz])

    def prod(buf, rows, dz):
        return lax.dot_general(buf[:, slab(dz)], a_v[rows, slab(dz)], NT, preferred_element_type=F32)

    own = jnp.zeros((16, B), F32)
    far = jnp.zeros((16, B), F32)
    for dz in NEAR[:-1]:
        wait_slab(y1_v, 0, dz)
        far = far + prod(y1_v, theirs, dz)
        own = own + prod(y1_v, mine, dz)
    dz = NEAR[-1]
    wait_slab(y1_v, 0, dz)
    z1_v[...] = far + prod(y1_v, theirs, dz)
    zc = rcopy(z1_v, z1_rx, d_send.at[0], d_recv.at[0], partner)
    zc.start()
    own = own + prod(y1_v, mine, dz)
    zc.wait()
    z1 = own + z1_rx[...]
    h_bf = jnp.maximum(z1, 0.0).astype(BF)
    rows16 = lax.broadcasted_iota(jnp.int32, (16, B), 0)
    y2 = jnp.dot(wo_bf, h_bf, preferred_element_type=F32)
    y2 = jnp.where(rows16 == CLS, tm_v[:, mine].astype(F32), y2)
    y2_v[:, blk(chip)] = y2.astype(BF)
    gather_start(y2_v, 1)

    lc.wait()
    mc.wait()
    every = slice(0, 2 * B)
    both = jnp.zeros((16, 2 * B), F32)
    cnt = jnp.zeros((16, B), F32)

    def slab_count(dz, cnt):
        z = lax.rem(cz + R - dz, R)
        for t in range(SL):
            cnt = cnt + y2_v[:, blk(z * SL + t)].astype(F32)
        return cnt

    for dz in NEAR[:-1]:
        wait_slab(y2_v, 1, dz)
        both = both + prod(y2_v, every, dz)
        cnt = slab_count(dz, cnt)
    dz = NEAR[-1]
    wait_slab(y2_v, 1, dz)
    both = both + prod(y2_v, every, dz)
    cnt = slab_count(dz, cnt)
    for h in range(2):
        z2_v[:, h * B:(h + 1) * B] = jnp.where(rows16 == CLS, cnt, both[:, h * B:(h + 1) * B])
    zc2 = rcopy(z2_v, z2_rx, d_send.at[1], d_recv.at[1], partner)
    zc2.start()
    zc2.wait()
    z2 = (z2_v[...] + z2_rx[...])[0:8, :]
    rows8 = lax.broadcasted_iota(jnp.int32, (8, 2 * B), 0)
    lanes = lax.broadcasted_iota(jnp.int32, (1, 2 * B), 1)
    count = jnp.sum(z2[CLS:CLS + 1, 0:B], axis=1, keepdims=True)
    m_row = tm_v[...].astype(F32)
    valid = rows8 < CLS
    zmax = jnp.max(jnp.where(valid, z2, -jnp.inf), axis=0, keepdims=True)
    esum = jnp.sum(jnp.where(valid, jnp.exp(jnp.where(valid, z2 - zmax, 0.0)), 0.0), axis=0, keepdims=True)
    log_norm = jnp.log(esum) + zmax
    hot = rows8 == lab_v[...]
    picked = jnp.sum(jnp.where(hot, z2, 0.0), axis=0, keepdims=True)
    loss_row = jnp.where(lax.div(lanes, B) == core, m_row * (log_norm - picked), 0.0)
    loss_part = jnp.sum(loss_row, axis=1, keepdims=True)
    prob = jnp.exp(jnp.where(valid, z2 - log_norm, 0.0))
    g = (prob - hot.astype(F32)) * (m_row / count)
    g = jnp.where(valid, g, 0.0)
    g_v[...] = jnp.concatenate([g, jnp.zeros_like(g)], axis=0).astype(BF)

    def scatter_product(lhs_v, rows, out_v, rx, i):
        lhs = lhs_v[...]
        for dz in FAR:
            base = tz[dz]
            res = jnp.dot(lhs, a_v[:, pl.ds(pl.multiple_of(base * B, SL * B), SL * B)], preferred_element_type=F32)
            for j in range(SL):
                out_v[base + j] = res[0:rows, j * B:(j + 1) * B]
            for dy in FAR:
                for dx in FAR:
                    if dz or dy or dx:
                        rcopy(out_v.at[base + ty[dy] + tx[dx]], rx.at[chip], send_sem.at[i], recv_sem.at[i, 0], dev(dz, dy, dx)).start()
        rx[chip] = out_v[chip]

    def scatter_sum(rx, i):
        wait_all(rx.at[0:NC - 1], recv_sem.at[i, 0])
        return jnp.sum(rx[...], axis=0)

    scatter_product(g_v, 8, p_v, p_rx, 2)
    d2 = scatter_sum(p_rx, 2)
    d2_16 = jnp.concatenate([d2, jnp.zeros((8, B), F32)], axis=0).astype(BF)
    gh = lax.dot_general(wo_bf, d2_16, TN, preferred_element_type=F32)
    e_v[:, mine] = jnp.where(z1 > 0, gh, 0.0).astype(BF)
    ec = rcopy(e_v.at[:, mine], e_v.at[:, mine], d_send.at[2], d_recv.at[2], partner)
    ec.start()
    gwo = lax.dot_general(d2_16, h_bf, NT, preferred_element_type=F32)
    for h in range(2):
        part[h, :, fpad:fpad + 16] = jnp.where(rows8[:, 0:16] == CLS, loss_part, gwo[0:8, :])
    ec.wait()
    scatter_product(e_v, 16, q_v, q_rx, 3)
    d1 = scatter_sum(q_rx, 3).astype(BF)
    gwh = lax.dot_general(d1, x_v[...], NT, preferred_element_type=F32)
    part[0, :, 0:f_in] = gwh[0:8]
    part[1, :, 0:f_in] = gwh[8:16]

    third = width // B // 3 * B
    cuts = [slice(0, third), slice(third, 2 * third), slice(2 * third, width)]

    def launch(p, s):
        ax = (p + s) % 3
        c = cuts[s]
        me_ax = coords[ax]
        ss, rs = ar_send.at[p, s], ar_recv.at[p, s]
        for d in FAR:
            if p == 1:
                if d:
                    rcopy(acc1.at[:, c], rx1.at[me_ax, :, c], ss, rs, ring_dev(ax, d, core)).start()
                continue
            for h in (other, core):
                if d == 0 and h is core:
                    continue
                src = part.at[h, :, c] if p == 0 else acc2.at[:, c]
                slot = me_ax * 2 + core if p == 0 else core * R + me_ax
                rcopy(src, (rx0 if p == 0 else rx2).at[slot, :, c], ss, rs, ring_dev(ax, d, h)).start()
        if p == 0:
            rx0[me_ax * 2 + core, :, c] = part[core, :, c]
        elif p == 1:
            rx1[me_ax, :, c] = acc1[:, c]
        else:
            rx2[core * R + me_ax, :, c] = acc2[:, c]

    def total(rx, lo, n, c):
        tot = rx[lo, :, c]
        for r in range(1, n):
            tot = tot + rx[lo + r, :, c]
        return tot

    for s in range(3):
        launch(0, s)
    for s in range(3):
        c = cuts[s]
        wait_all(rx0.at[0:2 * R - 1, :, c], ar_recv.at[0, s])
        acc1[:, c] = total(rx0, 0, 2 * R, c)
        launch(1, s)
    for s in range(3):
        c = cuts[s]
        wait_all(rx1.at[0:R - 1, :, c], ar_recv.at[1, s])
        acc2[:, c] = total(rx1, 0, R, c)
        launch(2, s)
    for s in range(3):
        c = cuts[s]
        wait_all(rx2.at[0:2 * R - 1, :, c], ar_recv.at[2, s])
        end = min(c.stop, f_in)
        lo = total(rx2, 0, R, c)
        hi = total(rx2, R, R, c)
        gwh_out[0:8, c.start:end] = lo[:, 0:end - c.start]
        gwh_out[8:16, c.start:end] = hi[:, 0:end - c.start]
        if s == 2:
            tail = lo[:, fpad - c.start:]
            gwo_out[...] = tail[0:CLS, 0:16]
            loss_out[...] = tail[CLS:CLS + 1, 0:1] / count

    wait_all(a_v.at[0:B, :], a_send)
    wait_all(y1_v.at[:, 0:(NC - 1) * B], send_sem.at[0])
    wait_all(y2_v.at[:, 0:(NC - 1) * B], send_sem.at[1])
    wait_all(p_rx.at[0:NC - 1], send_sem.at[2])
    wait_all(q_rx.at[0:NC - 1], send_sem.at[3])
    for s in range(3):
        c = cuts[s]
        wait_all(rx0.at[0:2 * R - 1, :, c], ar_send.at[0, s])
        wait_all(rx1.at[0:R - 1, :, c], ar_send.at[1, s])
        wait_all(rx2.at[0:2 * R - 1, :, c], ar_send.at[2, s])


def device_step(R, adj, feat, w_hidden, w_output, labels, train_mask, block_mask):
    NC = R * R * R
    f_in, hid = w_hidden.shape
    fpad = -(-f_in // B) * B
    any_spec = pl.BlockSpec(memory_space=pl.ANY)
    vmem_spec = pl.BlockSpec(memory_space=pltpu.VMEM)
    gwh, gwo, loss = pl.pallas_call(
        functools.partial(kernel, R),
        out_shape=(pltpu.VMEM((hid, f_in), F32), pltpu.VMEM((CLS, hid), F32), pltpu.VMEM((1, 1), F32)),
        in_specs=[any_spec] * 7,
        out_specs=(vmem_spec, vmem_spec, vmem_spec),
        scratch_shapes=[
            pltpu.VMEM((2 * B, NC * B), BF),
            pltpu.VMEM((f_in, B), BF),
            pltpu.VMEM((hid, f_in), F32),
            pltpu.VMEM((CLS, hid), F32),
            pltpu.VMEM((16, hid), F32),
            pltpu.VMEM((1, 2 * B), jnp.int32),
            pltpu.VMEM((1, 2 * B), jnp.int32),
            pltpu.SMEM((8, block_mask.shape[1]), jnp.int32),
            pltpu.VMEM((hid, NC * B), BF),
            pltpu.VMEM((16, NC * B), BF),
            pltpu.VMEM((16, B), F32),
            pltpu.VMEM((16, B), F32),
            pltpu.VMEM((16, 2 * B), F32),
            pltpu.VMEM((16, 2 * B), F32),
            pltpu.VMEM((16, 2 * B), BF),
            pltpu.VMEM((16, 2 * B), BF),
            pltpu.VMEM((NC, 8, B), F32),
            pltpu.VMEM((NC, 8, B), F32),
            pltpu.VMEM((NC, 16, B), F32),
            pltpu.VMEM((NC, 16, B), F32),
            pltpu.VMEM((2, 8, fpad + B), F32),
            pltpu.VMEM((2 * R, 8, fpad + B), F32),
            pltpu.VMEM((8, fpad + B), F32),
            pltpu.VMEM((R, 8, fpad + B), F32),
            pltpu.VMEM((8, fpad + B), F32),
            pltpu.VMEM((2 * R, 8, fpad + B), F32),
            pltpu.SemaphoreType.DMA((6,)),
            pltpu.SemaphoreType.DMA((2,)),
            pltpu.SemaphoreType.DMA,
            pltpu.SemaphoreType.DMA((5,)),
            pltpu.SemaphoreType.DMA((5,)),
            pltpu.SemaphoreType.DMA((4,)),
            pltpu.SemaphoreType.DMA((4, R)),
            pltpu.SemaphoreType.DMA((3, 3)),
            pltpu.SemaphoreType.DMA((3, 3)),
        ],
        compiler_params=pltpu.CompilerParams(collective_id=0, has_side_effects=True, vmem_limit_bytes=60 * 1024 * 1024),
        name='gcn_step',
    )(adj, feat.T, w_hidden.T, w_output.T, labels.reshape(1, -1), train_mask.reshape(1, -1), block_mask)
    return loss[0, 0], gwh.T, gwo.T


def solution(mesh):
    row_spec = P(AXIS, None)
    vec_spec = P(AXIS)
    R = 4 if mesh.shape[AXIS] == 128 else 2
    return jax.shard_map(functools.partial(device_step, R), mesh=mesh,
                         in_specs=(row_spec, row_spec, P(), P(), vec_spec, vec_spec, P()), out_specs=(P(), P(), P()), check_vma=False)
```

```python
import functools

import jax
import jax.numpy as jnp
from jax import lax
from jax.experimental import pallas as pl
from jax.experimental.pallas import tpu as pltpu
from jax.sharding import PartitionSpec as P

AXIS = 'nodes'
MESH = pl.DeviceIdType.MESH
BF = jnp.bfloat16
F32 = jnp.float32
NT = (((1,), (1,)), ((), ()))
TN = (((0,), (0,)), ((), ()))
B = 128
CLS = 7


def tail_offset(f_in):
    return -(-f_in // 16) * 16


def kernel(R, adj, x_t, wh_t, wo_t, labels, tmask, bmask, out,
           a_v, x_v, wh_v, wo_v, wo_pad, lab_v, tm_v, bm_s, y1_v, y2_v, z1_v, z1_rx, z2_v, z2_rx,
           g_v, e_v, p_v, p_rx, q_v, q_rx, part, rx0, acc1, rx1, acc2, rx2,
           load_sem, a_sem, a_send, d_send, d_recv, send_sem, recv_sem, ar_send, ar_recv):
    NC = R * R * R
    SL = R * R
    FAR = (2, 3, 1, 0) if R == 4 else (1, 0)
    NEAR = FAR[::-1]
    f_in = x_v.shape[0]
    width = part.shape[2]
    toff = tail_offset(f_in)
    tail = slice(toff, toff + 16)
    me = lax.axis_index(AXIS)
    core = lax.rem(me, 2)
    other = 1 - core
    chip = lax.div(me, 2)
    cx = lax.rem(chip, R)
    cy = lax.rem(lax.div(chip, R), R)
    cz = lax.div(chip, SL)
    coords = (cz, cy, cx)
    partner = chip * 2 + other
    tz = [lax.rem(cz + d, R) * SL for d in range(R)]
    ty = [lax.rem(cy + d, R) * R for d in range(R)]
    tx = [lax.rem(cx + d, R) for d in range(R)]
    offsets = [(dz, dy, dx) for dz in FAR for dy in FAR for dx in FAR if dz or dy or dx]
    offsets.sort(key=lambda o: -sum(min(d, R - d) for d in o))
    tz_src = [lax.rem(cz + R - d, R) * SL for d in range(R)]
    ty_src = [lax.rem(cy + R - d, R) * R for d in range(R)]

    def rank_of(o):
        return max(sum(min(d, R - d) for d in o[:2]) - 1, 0)

    ranks = [[(dz, dy) for dz in range(R) for dy in range(R) if rank_of((dz, dy)) == r] for r in range(2 * (R // 2))]
    arrivals = [R * len(r) - (1 if (0, 0) in r else 0) for r in ranks]
    dz2 = [t * 2 + core for t in tz]
    dy2 = [t * 2 for t in ty]
    dx2 = [t * 2 for t in tx]

    def dev(dz, dy, dx):
        return dz2[dz] + dy2[dy] + dx2[dx]

    def blk(t):
        return pl.ds(pl.multiple_of(t * B, B), B)

    def rcopy(src, dst, ss, rs, device):
        return pltpu.make_async_remote_copy(src_ref=src, dst_ref=dst, send_sem=ss, recv_sem=rs, device_id=(device,), device_id_type=MESH)

    def wait_all(ref, sem):
        pltpu.make_async_copy(ref, ref, sem).wait()

    def ring_dev(ax, d, h):
        off = [0, 0, 0]
        off[ax] = d
        return (tz[off[0]] + ty[off[1]] + tx[off[2]]) * 2 + h

    barrier = pltpu.get_barrier_semaphore()
    for o in offsets:
        pl.semaphore_signal(barrier, inc=1, device_id=(dev(*o),), device_id_type=MESH)
    pl.semaphore_signal(barrier, inc=1, device_id=(partner,), device_id_type=MESH)
    for ax in range(3):
        for d in range(1, R):
            pl.semaphore_signal(barrier, inc=1, device_id=(ring_dev(ax, d, other),), device_id_type=MESH)

    mine = blk(core)
    theirs = blk(other)
    small = [
        pltpu.make_async_copy(x_t, x_v, load_sem.at[0]),
        pltpu.make_async_copy(wh_t, wh_v, load_sem.at[1]),
        pltpu.make_async_copy(bmask.at[pl.ds(pl.multiple_of(lax.div(2 * chip, 8) * 8, 8), 8), :], bm_s, load_sem.at[2]),
        pltpu.make_async_copy(wo_t, wo_v, load_sem.at[3]),
        pltpu.make_async_copy(labels, lab_v.at[:, mine], load_sem.at[4]),
        pltpu.make_async_copy(tmask, tm_v.at[:, mine], load_sem.at[5]),
    ]
    for c in small:
        c.start()

    def load_a(t, _):
        pltpu.make_async_copy(adj.at[:, blk(2 * t + core)], a_v.at[mine, blk(t)], a_sem.at[0]).start()
        return 0

    lax.fori_loop(0, NC, load_a, 0, unroll=4)
    wo_pad[...] = jnp.zeros_like(wo_pad)
    part[...] = jnp.zeros_like(part)
    small[0].wait()
    small[1].wait()
    y1_v[:, blk(chip)] = jnp.dot(wh_v[...].astype(BF), x_v[...], preferred_element_type=F32).astype(BF)
    for c in small[2:]:
        c.wait()
    wo_pad[0:CLS, :] = wo_v[...]
    wo_bf = wo_pad[...].astype(BF)

    row0 = lax.rem(2 * chip, 8)

    def mask_rows(h):
        def step(t, _):
            m = jnp.full((B, B), bm_s[row0 + h, 2 * t + core].astype(F32), F32).astype(BF)
            a_v[blk(h), blk(t)] = a_v[blk(h), blk(t)] * m
            return 0

        lax.fori_loop(0, NC, step, 0, unroll=4)

    wait_all(a_v.at[0:B, :], a_sem.at[0])
    mask_rows(core)

    pl.semaphore_wait(barrier, NC + 3 * (R - 1))

    def gather_start(buf, i):
        src = buf.at[:, blk(chip)]
        for o in offsets:
            rcopy(src, src, send_sem.at[i], recv_sem.at[i, rank_of(o)], dev(*o)).start()

    gather_start(y1_v, 0)

    def swap_a(t, _):
        rcopy(adj.at[:, blk(2 * t + other)], a_v.at[mine, blk(t)], a_send, a_sem.at[1], partner).start()
        return 0

    lax.fori_loop(0, NC, swap_a, 0, unroll=4)
    lc = rcopy(labels, lab_v.at[:, mine], d_send.at[3], d_recv.at[3], partner)
    mc = rcopy(tmask, tm_v.at[:, mine], d_send.at[4], d_recv.at[4], partner)
    lc.start()
    mc.start()
    wait_all(a_v.at[0:B, :], a_sem.at[1])
    mask_rows(other)

    def group(o):
        return pl.ds(pl.multiple_of((tz_src[o[0]] + ty_src[o[1]]) * B, R * B), R * B)

    def wait_rank(buf, i, rank):
        wait_all(buf.at[:, 0:arrivals[rank] * B], recv_sem.at[i, rank])

    def prod(buf, rank):
        left = jnp.concatenate([buf[:, group(o)] for o in rank], axis=1)
        halves = []
        for h in range(2):
            right = jnp.concatenate([a_v[h * B:(h + 1) * B, group(o)] for o in rank], axis=1)
            halves.append(lax.dot_general(left, right, NT, preferred_element_type=F32))
        return halves

    def gathered_product(buf, i, counted=False):
        cnt = jnp.zeros((buf.shape[0], B), F32)
        lo = jnp.zeros((buf.shape[0], B), F32)
        hi = jnp.zeros((buf.shape[0], B), F32)
        for rank in range(len(ranks)):
            wait_rank(buf, i, rank)
            p_lo, p_hi = prod(buf, ranks[rank])
            lo = lo + p_lo
            hi = hi + p_hi
            if counted:
                for o in ranks[rank]:
                    for x in range(R):
                        cnt = cnt + buf[:, blk(tz_src[o[0]] + ty_src[o[1]] + x)].astype(F32)
        return (lo, hi, cnt) if counted else (lo, hi)

    z1_v[0], z1_v[1] = gathered_product(y1_v, 0)
    zc = rcopy(z1_v.at[other], z1_rx, d_send.at[0], d_recv.at[0], partner)
    zc.start()
    zc.wait()
    z1 = z1_v[core] + z1_rx[...]
    h_bf = jnp.maximum(z1, 0.0).astype(BF)
    rows8 = lax.broadcasted_iota(jnp.int32, (8, 2 * B), 0)
    is_count = rows8[:, 0:B] == CLS
    y2 = jnp.dot(wo_bf, h_bf, preferred_element_type=F32)
    y2 = jnp.where(is_count, tm_v[:, mine].astype(F32), y2)
    y2_v[:, blk(chip)] = y2.astype(BF)
    gather_start(y2_v, 1)

    lc.wait()
    mc.wait()
    *both, cnt = gathered_product(y2_v, 1, counted=True)
    for h in range(2):
        z2_v[:, h * B:(h + 1) * B] = jnp.where(is_count, cnt, both[h])
    zc2 = rcopy(z2_v, z2_rx, d_send.at[1], d_recv.at[1], partner)
    zc2.start()
    zc2.wait()
    z2 = z2_v[...] + z2_rx[...]
    lanes = lax.broadcasted_iota(jnp.int32, (1, 2 * B), 1)
    count = jnp.sum(z2[CLS:CLS + 1, 0:B], axis=1, keepdims=True)
    m_row = tm_v[...].astype(F32)
    valid = rows8 < CLS
    zmax = jnp.max(jnp.where(valid, z2, -jnp.inf), axis=0, keepdims=True)
    esum = jnp.sum(jnp.where(valid, jnp.exp(jnp.where(valid, z2 - zmax, 0.0)), 0.0), axis=0, keepdims=True)
    log_norm = jnp.log(esum) + zmax
    hot = rows8 == lab_v[...]
    picked = jnp.sum(jnp.where(hot, z2, 0.0), axis=0, keepdims=True)
    loss_row = jnp.where(lax.div(lanes, B) == core, m_row * (log_norm - picked), 0.0)
    loss_part = jnp.sum(loss_row, axis=1, keepdims=True)
    prob = jnp.exp(jnp.where(valid, z2 - log_norm, 0.0))
    g = (prob - hot.astype(F32)) * (m_row / count)
    g_v[...] = jnp.where(valid, g, 0.0).astype(BF)

    def product(lhs, rings):
        cols = jnp.concatenate([a_v[:, pl.ds(pl.multiple_of((tz[o[0]] + ty[o[1]]) * B, R * B), R * B)] for o in rings], axis=1)
        return jnp.dot(lhs, cols, preferred_element_type=F32)

    def scatter_product(lhs_v, outs, chunks, send_block):
        lhs = lhs_v[...]
        for chunk in chunks:
            cut = (len(chunk) + 1) // 2
            for rings in (chunk[:cut], chunk[cut:]):
                if rings:
                    res = product(lhs, rings)
                    for n, o in enumerate(rings):
                        for j in range(R):
                            for h, out_v in enumerate(outs):
                                out_v[tz[o[0]] + ty[o[1]] + j] = res[h * 8:h * 8 + 8, (n * R + j) * B:(n * R + j + 1) * B]
            for o in offsets:
                if o[:2] in chunk:
                    send_block(0, o)

    def sender(outs, rxs, i):
        def send_block(h, o):
            t = tz[o[0]] + ty[o[1]] + tx[o[2]]
            rcopy(outs[h].at[t], rxs[h].at[chip], send_sem.at[i + h], recv_sem.at[i + h, 0], dev(*o)).start()

        return send_block

    def scatter_sum(rx, i):
        wait_all(rx.at[0:NC - 1], recv_sem.at[i, 0])
        return jnp.sum(rx[...], axis=0)

    by_rank = [list(r) for r in ranks[::-1]]
    if R == 4:
        by_rank = [by_rank[0] + by_rank[1], by_rank[2], by_rank[3]]
    by_z = [[(dz, dy) for dy in FAR] for dz in FAR]

    scatter_product(g_v, [p_v], by_rank, sender([p_v], [p_rx], 2))
    p_rx[chip] = p_v[chip]
    d2 = scatter_sum(p_rx, 2).astype(BF)
    gh = lax.dot_general(wo_bf, d2, TN, preferred_element_type=F32)
    e_v[:, mine] = jnp.where(z1 > 0, gh, 0.0).astype(BF)
    ec = rcopy(e_v.at[:, mine], e_v.at[:, mine], d_send.at[2], d_recv.at[2], partner)
    ec.start()
    gwo = lax.dot_general(d2, h_bf, NT, preferred_element_type=F32)
    ec.wait()
    q_vs = [q_v.at[h] for h in range(2)]
    q_rxs = [q_rx.at[h] for h in range(2)]
    send_q = sender(q_vs, q_rxs, 3)
    scatter_product(e_v, q_vs, by_z, send_q)
    for o in offsets:
        send_q(1, o)
    for h in range(2):
        q_rx[h, chip] = q_v[h, chip]

    tiles = width // B
    streams = 6 if tiles >= 6 else 3
    cuts = [slice(tiles * s // streams * B, tiles * (s + 1) // streams * B) for s in range(streams)]

    def launch_first(h, s):
        ax = s % 3
        c = cuts[s]
        slot = coords[ax] * 2 + core
        for d in FAR[:-1]:
            rcopy(part.at[h, :, c], rx0.at[slot, :, c], ar_send.at[0, s], ar_recv.at[0, s], ring_dev(ax, d, h)).start()

        @pl.when(core == h)
        def _():
            rx0[slot, :, c] = part[h, :, c]

        @pl.when(core != h)
        def _():
            rcopy(part.at[h, :, c], rx0.at[slot, :, c], ar_send.at[0, s], ar_recv.at[0, s], partner).start()

    def launch(p, s):
        ax = (p + s) % 3
        c = cuts[s]
        me_ax = coords[ax]
        ss, rs = ar_send.at[p, s], ar_recv.at[p, s]
        for d in FAR:
            if p == 1:
                if d:
                    rcopy(acc1.at[:, c], rx1.at[me_ax, :, c], ss, rs, ring_dev(ax, d, core)).start()
                continue
            for h in (other, core):
                if d or h is other:
                    rcopy(acc2.at[:, c], rx2.at[core * R + me_ax, :, c], ss, rs, ring_dev(ax, d, h)).start()
        if p == 1:
            rx1[me_ax, :, c] = acc1[:, c]
        else:
            rx2[core * R + me_ax, :, c] = acc2[:, c]

    def total(rx, lo, n, c):
        tot = rx[lo, :, c]
        for r in range(1, n):
            tot = tot + rx[lo + r, :, c]
        return tot

    for h in range(2):
        d1 = scatter_sum(q_rxs[h], 3 + h).astype(BF)
        part[h, :, 0:f_in] = lax.dot_general(d1, x_v[...], NT, preferred_element_type=F32)
        part[h, :, tail] = jnp.where(rows8[:, 0:16] == CLS, loss_part, gwo)
        for s in range(streams):
            launch_first(h, s)
    for s in range(streams):
        c = cuts[s]
        wait_all(rx0.at[0:2 * R - 1, :, c], ar_recv.at[0, s])
        acc1[:, c] = total(rx0, 0, 2 * R, c)
        launch(1, s)
    for s in range(streams):
        c = cuts[s]
        wait_all(rx1.at[0:R - 1, :, c], ar_recv.at[1, s])
        acc2[:, c] = total(rx1, 0, R, c)
        launch(2, s)
    for s in range(streams):
        c = cuts[s]
        wait_all(rx2.at[0:2 * R - 1, :, c], ar_recv.at[2, s])
        out[0:8, c] = total(rx2, 0, R, c)
        out[8:16, c] = total(rx2, R, R, c)
    out[15:16, tail] = jnp.broadcast_to(out[CLS:CLS + 1, toff:toff + 1] / count, (1, 16))

    wait_all(a_v.at[0:B, :], a_send)
    wait_all(y1_v.at[:, 0:(NC - 1) * B], send_sem.at[0])
    wait_all(y2_v.at[:, 0:(NC - 1) * B], send_sem.at[1])
    wait_all(p_rx.at[0:NC - 1], send_sem.at[2])
    for h in range(2):
        wait_all(q_rx.at[h, 0:NC - 1], send_sem.at[3 + h])
    for s in range(streams):
        c = cuts[s]
        wait_all(rx0.at[0:2 * R - 1, :, c], ar_send.at[0, s])
        wait_all(rx1.at[0:R - 1, :, c], ar_send.at[1, s])
        wait_all(rx2.at[0:2 * R - 1, :, c], ar_send.at[2, s])


def unpack(packed, gwh_out, gwo_out, loss_out):
    f_in = gwh_out.shape[1]
    toff = tail_offset(f_in)
    gwh_out[...] = packed[:, 0:f_in]
    gwo_out[...] = packed[0:CLS, toff:toff + 16]
    loss_out[...] = packed[15:16, toff:toff + 1]


def device_step(R, adj, feat, w_hidden, w_output, labels, train_mask, block_mask):
    NC = R * R * R
    f_in, hid = w_hidden.shape
    width = -(-(tail_offset(f_in) + 16) // B) * B
    any_spec = pl.BlockSpec(memory_space=pl.ANY)
    vmem_spec = pl.BlockSpec(memory_space=pltpu.VMEM)
    packed = pl.pallas_call(
        functools.partial(kernel, R),
        out_shape=pltpu.VMEM((hid, width), F32),
        in_specs=[any_spec] * 7,
        out_specs=vmem_spec,
        scratch_shapes=[
            pltpu.VMEM((2 * B, NC * B), BF),
            pltpu.VMEM((f_in, B), BF),
            pltpu.VMEM((hid, f_in), F32),
            pltpu.VMEM((CLS, hid), F32),
            pltpu.VMEM((8, hid), F32),
            pltpu.VMEM((1, 2 * B), jnp.int32),
            pltpu.VMEM((1, 2 * B), jnp.int32),
            pltpu.SMEM((8, block_mask.shape[1]), jnp.int32),
            pltpu.VMEM((hid, NC * B), BF),
            pltpu.VMEM((8, NC * B), BF),
            pltpu.VMEM((2, 16, B), F32),
            pltpu.VMEM((16, B), F32),
            pltpu.VMEM((8, 2 * B), F32),
            pltpu.VMEM((8, 2 * B), F32),
            pltpu.VMEM((8, 2 * B), BF),
            pltpu.VMEM((16, 2 * B), BF),
            pltpu.VMEM((NC, 8, B), F32),
            pltpu.VMEM((NC, 8, B), F32),
            pltpu.VMEM((2, NC, 8, B), F32),
            pltpu.VMEM((2, NC, 8, B), F32),
            pltpu.VMEM((2, 8, width), F32),
            pltpu.VMEM((2 * R, 8, width), F32),
            pltpu.VMEM((8, width), F32),
            pltpu.VMEM((R, 8, width), F32),
            pltpu.VMEM((8, width), F32),
            pltpu.VMEM((2 * R, 8, width), F32),
            pltpu.SemaphoreType.DMA((6,)),
            pltpu.SemaphoreType.DMA((2,)),
            pltpu.SemaphoreType.DMA,
            pltpu.SemaphoreType.DMA((5,)),
            pltpu.SemaphoreType.DMA((5,)),
            pltpu.SemaphoreType.DMA((5,)),
            pltpu.SemaphoreType.DMA((5, R)),
            pltpu.SemaphoreType.DMA((3, 6)),
            pltpu.SemaphoreType.DMA((3, 6)),
        ],
        compiler_params=pltpu.CompilerParams(collective_id=0, has_side_effects=True, vmem_limit_bytes=60 * 1024 * 1024),
        name='gcn_step',
    )(adj, feat.T, w_hidden.T, w_output.T, labels.reshape(1, -1), train_mask.reshape(1, -1), block_mask)
    gwh, gwo, loss = pl.pallas_call(
        unpack,
        out_shape=(jax.ShapeDtypeStruct((hid, f_in), F32), jax.ShapeDtypeStruct((CLS, hid), F32), jax.ShapeDtypeStruct((1, 1), F32)),
        in_specs=[vmem_spec],
        out_specs=(vmem_spec, vmem_spec, vmem_spec),
        name='gcn_unpack',
    )(pltpu.with_memory_space_constraint(packed, pltpu.VMEM))
    return loss[0, 0], gwh.T, gwo.T


def solution(mesh):
    row_spec = P(AXIS, None)
    vec_spec = P(AXIS)
    R = 4 if mesh.shape[AXIS] == 128 else 2
    return jax.shard_map(functools.partial(device_step, R), mesh=mesh,
                         in_specs=(row_spec, row_spec, P(), P(), vec_spec, vec_spec, P()), out_specs=(P(), P(), P()), check_vma=False)
```
